32 devices in a mesh: rad: 8 (over y, x, core), az: 4 (over z).
Axes of the slice: x: 2, y: 2, z: 4, core: 2. Of those that a mesh axis runs over, the one named last changes fastest.
Arguments:
- surface_mass: float32 [256, 16384], P('rad', 'az'), may hold values from 0.5 to 2
- outward_drift: float32 [256, 16384], P('rad', 'az'), may hold values from -1.2 to 1.2
- leftover_angular_drift: float32 [256, 16384], P('rad', 'az'), may hold values from -1.2 to 1.2
- angular_offsets: int32 [256], P('rad'), may hold values from 0 to 16383
- planetesimal_loop_number: int32 [32], replicated, may hold values from 0 to 255
- planetesimal_angle_bin: int32 [32], replicated, may hold values from 0 to 16383
- planetesimal_weights: float32 [32], replicated, may hold values from 0.001 to 0.01
Outputs:
- transported_density: float32 [256, 16384], P('rad', 'az')
- kicked_radial_velocity: float32 [256, 16384], P('rad', 'az')
- kicked_azimuthal_velocity: float32 [256, 16384], P('rad', 'az')
- embryo_disk_acceleration: float32 [2, 32], replicated
The draws below stay inside these ranges and needn't reach their ends.
All inputs are finite; a program needn't handle non-finite values.
Results may differ from the reference program's by a relative error of at most 0.0003.
Values sent between devices are 32-bit elements; how exact they have to be, the bound alone decides.
A program may use at most 64 MiB of HBM per device.

```python
import math
import jax
import jax.numpy as jnp
from jax import lax

ANGULAR_BINS = 16384
MODES = 256
EMB = 32
LOOP_COUNT = 256


def place_ends(array, rng, least, top_value):
    longest = array.shape.index(max(array.shape))
    spots = []
    for shift in (0, 1):
        where = [jax.random.randint(jax.random.fold_in(rng, axis), (), 0, length) for axis, length in enumerate(array.shape)]
        where[longest] = (where[longest] + shift) % array.shape[longest]
        spots.append(tuple(where))
    return array.at[spots[0]].set(least).at[spots[1]].set(top_value)


def level_of(stream_key, extent, cuts, smallest, top_value):
    gain = 1.0
    for axis_at, shards_of in cuts:
        heights = jax.random.uniform(jax.random.fold_in(jax.random.fold_in(stream_key, 6), axis_at), (shards_of,), jnp.float32, smallest / len(cuts), top_value / len(cuts))
        gain = gain * jnp.repeat(jnp.exp(heights), extent[axis_at] // shards_of).reshape((-1,) + (1,) * (len(extent) - 1 - axis_at))
    return gain


def centred(key, extent, deviation, most, shards=(), kind=jnp.bfloat16):
    entries = jax.random.normal(key, extent, jnp.float32) * deviation
    if len(shards) > 0:
        entries = level_of(key, extent, shards, -0.22, 0.18) * entries
    return jnp.clip(entries, min=-most, max=most).astype(kind)


def setup_inputs(seed: int = 0) -> dict:
    streams_of = jax.random.split(jax.random.key(seed), 8)
    surface_mass = jnp.clip(jnp.exp(math.log(2.0) - 1.3862944 * jax.random.uniform(streams_of[0], (LOOP_COUNT, ANGULAR_BINS), jnp.float32) ** level_of(streams_of[0], (LOOP_COUNT, ANGULAR_BINS), ((0, 8), (1, 4)), -0.2, 0.2)), 0.5, 2.0)
    outward_drift = centred(streams_of[1], (LOOP_COUNT, ANGULAR_BINS), 0.3, 1.2, ((0, 8), (1, 4)), jnp.float32)
    leftover_angular_drift = centred(streams_of[2], (LOOP_COUNT, ANGULAR_BINS), 0.3, 1.2, ((0, 8), (1, 4)), jnp.float32)
    angular_offsets = place_ends(jax.random.randint(streams_of[3], (LOOP_COUNT,), 0, ANGULAR_BINS), jax.random.fold_in(streams_of[3], 1), 0, ANGULAR_BINS - 1).astype(jnp.int32)
    planetesimal_loop_number = place_ends(jax.random.randint(streams_of[4], (EMB,), 0, LOOP_COUNT), jax.random.fold_in(streams_of[4], 1), 0, LOOP_COUNT - 1).astype(jnp.int32)
    planetesimal_angle_bin = place_ends(jax.random.randint(streams_of[5], (EMB,), 0, ANGULAR_BINS), jax.random.fold_in(streams_of[5], 1), 0, ANGULAR_BINS - 1).astype(jnp.int32)
    planetesimal_weights = jnp.clip(jnp.exp(jax.random.uniform(streams_of[6], (EMB,), jnp.float32, math.log(0.001), math.log(0.01))), 0.001, 0.01)
    return dict(surface_mass=surface_mass, outward_drift=outward_drift, leftover_angular_drift=leftover_angular_drift, angular_offsets=angular_offsets, planetesimal_loop_number=planetesimal_loop_number, planetesimal_angle_bin=planetesimal_angle_bin, planetesimal_weights=planetesimal_weights)


gravity = 1.0
timestep_length = 0.05
courant = 0.4
softening = 0.02

def mode_tables(first, count):
    columns = first + jnp.arange(count, dtype=jnp.int32)
    orders = jnp.arange(MODES, dtype=jnp.int32)
    phases = orders[:, None] * (2 * columns[None, :] + 1) % (2 * ANGULAR_BINS)
    angles = phases.astype(jnp.float32) * (jnp.pi / ANGULAR_BINS)
    return jnp.concatenate([jnp.cos(angles), jnp.sin(angles)], axis=0)

def column_angles(first, count):
    columns = first + jnp.arange(count, dtype=jnp.int32)
    return (2 * columns + 1).astype(jnp.float32) * (jnp.pi / ANGULAR_BINS)

def cycle_radius(first, count, cell_step):
    cycles = first + jnp.arange(count, dtype=jnp.int32)
    return jnp.exp((cycles.astype(jnp.float32) + 0.5) * cell_step)

def donor_flux(orbital_speeds, upstream, downstream):
    return jnp.where(orbital_speeds > 0, orbital_speeds * upstream, orbital_speeds * downstream)

def reference(surface_mass, outward_drift, leftover_angular_drift, angular_offsets, planetesimal_loop_number, planetesimal_angle_bin, planetesimal_weights):
    cycle_total = surface_mass.shape[0]
    cell_step = 2.0 * jnp.pi / ANGULAR_BINS
    highest = lax.Precision.HIGHEST
    columns = jnp.arange(ANGULAR_BINS, dtype=jnp.int32)
    upwind_surface_mass = (columns[None, :] - angular_offsets[:, None]) % ANGULAR_BINS
    single_density = jnp.take_along_axis(surface_mass, upwind_surface_mass, axis=1)
    single_radial_velocity = jnp.take_along_axis(outward_drift, upwind_surface_mass, axis=1)
    lone_angular_drift = jnp.take_along_axis(leftover_angular_drift, upwind_surface_mass, axis=1)
    orbital_speeds = 0.5 * (lone_angular_drift + jnp.roll(lone_angular_drift, -1, axis=1))
    fluxes = donor_flux(orbital_speeds, single_density, jnp.roll(single_density, -1, axis=1))
    dens_two = single_density - courant * (fluxes - jnp.roll(fluxes, 1, axis=1))
    orbital_speeds = 0.5 * (single_radial_velocity[:-1] + single_radial_velocity[1:])
    inner = donor_flux(orbital_speeds, dens_two[:-1], dens_two[1:])
    zero_row = jnp.zeros_like(inner[:1])
    fluxes = jnp.concatenate([zero_row, inner, zero_row], axis=0)
    transported_density = dens_two - courant * (fluxes[1:] - fluxes[:-1])
    tables = mode_tables(0, ANGULAR_BINS)
    spectra = jnp.einsum('rc,mc->rm', transported_density, tables, precision=highest) * cell_step
    decays = (jnp.arange(MODES, dtype=jnp.float32) + 0.5) * cell_step
    decays_both = jnp.concatenate([decays, decays])
    factor = jnp.exp(-decays_both)

    def sweep(carried, cycle_row):
        carried = cycle_row + factor * carried
        return (carried, carried)
    start = jnp.zeros_like(spectra[0])
    _, lower_sum = lax.scan(sweep, start, spectra)
    _, upper_sum = lax.scan(sweep, start, spectra[::-1])
    upper_sum = upper_sum[::-1]
    even_part = decays_both * (lower_sum + upper_sum - spectra)
    odd_part = decays_both * (lower_sum - upper_sum)
    orders = jnp.arange(MODES, dtype=jnp.float32)
    doubled = jnp.where(orders > 0, 2.0, 1.0)
    radial_weight = jnp.concatenate([doubled * decays, doubled * decays])
    azim_weight = jnp.concatenate([doubled * orders, -doubled * orders])
    radial_coef = odd_part * radial_weight
    azim_coef = jnp.concatenate([even_part[:, MODES:], even_part[:, :MODES]], axis=1) * azim_weight
    radius = cycle_radius(0, cycle_total, cell_step)
    radial_disk = -(gravity / cell_step) / radius[:, None] * jnp.dot(radial_coef, tables, precision=highest)
    azimuthal_disk_pull = gravity / radius[:, None] * jnp.dot(azim_coef, tables, precision=highest)
    cell_angles = column_angles(0, ANGULAR_BINS)
    cos_cell = jnp.cos(cell_angles)[None, :]
    sin_cell = jnp.sin(cell_angles)[None, :]
    embryo_angles = (2 * planetesimal_angle_bin + 1).astype(jnp.float32) * (jnp.pi / ANGULAR_BINS)
    embryo_radii = jnp.exp((planetesimal_loop_number.astype(jnp.float32) + 0.5) * cell_step)
    column_radius = radius[:, None]
    area = (radius * radius * cell_step * cell_step)[:, None]

    def visit(carried, member):
        embryo_radius, embryo_cos, embryo_sin, embryo_weight = member
        cos_gap = cos_cell * embryo_cos + sin_cell * embryo_sin
        sin_gap = sin_cell * embryo_cos - cos_cell * embryo_sin
        squared = column_radius * column_radius + embryo_radius * embryo_radius - 2.0 * column_radius * embryo_radius * cos_gap + softening * embryo_radius * (softening * embryo_radius)
        inverse = lax.rsqrt(squared)
        cubed = inverse * inverse * inverse
        pulled = embryo_weight * cubed
        radial_sum = carried[0] - pulled * (column_radius - embryo_radius * cos_gap)
        azim_sum = carried[1] - pulled * embryo_radius * sin_gap
        weighted = transported_density * area * cubed
        push_x = jnp.sum(weighted * (column_radius * cos_cell - embryo_radius * embryo_cos))
        push_y = jnp.sum(weighted * (column_radius * sin_cell - embryo_radius * embryo_sin))
        return ((radial_sum, azim_sum), jnp.stack([push_x, push_y]))
    initial = (jnp.zeros_like(transported_density), jnp.zeros_like(transported_density))
    members = (embryo_radii, jnp.cos(embryo_angles), jnp.sin(embryo_angles), planetesimal_weights)
    (radial_emb, azimuthal_embryo_pull), gravity_pushes = lax.scan(visit, initial, members)
    kicked_radial_velocity = single_radial_velocity + timestep_length * (radial_disk + radial_emb)
    kicked_azimuthal_velocity = lone_angular_drift + timestep_length * (azimuthal_disk_pull + azimuthal_embryo_pull)
    return (transported_density, kicked_radial_velocity, kicked_azimuthal_velocity, jnp.transpose(gravity_pushes))
```

```python
import jax
import jax.numpy as jnp
from jax import lax
from jax.experimental import pallas as pl
from jax.experimental.pallas import tpu as pltpu
from jax.sharding import PartitionSpec as P

ANGULAR_BINS = 16384
MODES = 256
LANES = 128

gravity = 1.0
timestep_length = 0.05
courant = 0.4
softening = 0.02

VMEM = pl.BlockSpec(memory_space=pltpu.VMEM)
SMEM = pl.BlockSpec(memory_space=pltpu.SMEM)
f32 = jnp.float32
bf16 = jnp.bfloat16


def call(body, outs, specs, scratch=(), flops=0):
    return pl.pallas_call(
        body,
        out_shape=outs,
        in_specs=specs,
        out_specs=jax.tree.map(lambda _: VMEM, outs),
        scratch_shapes=list(scratch),
        compiler_params=pltpu.CompilerParams(vmem_limit_bytes=48 * 1024 * 1024),
        cost_estimate=pl.CostEstimate(flops=flops, bytes_accessed=1 << 20, transcendentals=0),
    )


def gap(emb_ref, e, count, half_cos_ref, half_sin_ref):
    s = half_sin_ref[...] * emb_ref[3 * count + e] - half_cos_ref[...] * emb_ref[4 * count + e]
    return 2.0 * emb_ref[e] * (s * s)


def embryo_field(
    a_ref, b_ref, r_ref, emb_ref, cos_ref, sin_ref, hc_ref, hs_ref, rad_ref, azi_ref, p_ref, q_ref, k_ref
):
    count = p_ref.shape[0]

    def prepare(e, _):
        radius, cos_e, sin_e = emb_ref[e], emb_ref[count + e], emb_ref[2 * count + e]
        p_ref[e] = radius * (cos_ref[...] * cos_e + sin_ref[...] * sin_e)
        q_ref[e] = radius * (sin_ref[...] * cos_e - cos_ref[...] * sin_e)
        k_ref[e] = gap(emb_ref, e, count, hc_ref, hs_ref)
        return 0

    lax.fori_loop(0, count, prepare, 0)

    def row(i, _):
        def one(e, sums):
            s0, s1, s2 = sums
            p, q = p_ref[e], q_ref[e]
            inverse = lax.rsqrt(a_ref[i * count + e] + b_ref[i * count + e] * k_ref[e])
            t = inverse * inverse * inverse
            return s0 + t, s1 + t * p, s2 + t * q

        zero = jnp.zeros(p_ref.shape[1:], f32)
        s0, s1, s2 = lax.fori_loop(0, count, one, (zero, zero, zero), unroll=8)
        rad_ref[i] = s1 - r_ref[i] * s0
        azi_ref[i] = -s2
        return 0

    lax.fori_loop(0, rad_ref.shape[0], row, 0)


def shift_cycles(start_ref, g_ref, dens_ref, vrad_ref, vphi_ref, line_ref):
    rows, blocks = dens_ref.shape[:2]
    whole = g_ref.shape[2]
    total = whole * LANES
    extra = line_ref.shape[1] - whole
    lane = lax.broadcasted_iota(jnp.int32, (blocks, LANES), 1)

    def window(field, start):
        block = start // LANES
        rest = start % LANES
        first = pltpu.roll(line_ref[field, pl.ds(block, blocks), :], LANES - rest, 1)
        second = pltpu.roll(line_ref[field, pl.ds(block + 1, blocks), :], LANES - rest, 1)
        return jnp.where(lane < LANES - rest, first, second)

    def row(i, _):
        for field in range(3):
            line_ref[field, :whole] = g_ref[field, i]
            line_ref[field, whole:] = g_ref[field, i, :extra]
        here = start_ref[i]
        below = (here + total - 1) % total
        above = (here + 1) % total
        d, dm, dp = window(0, here), window(0, below), window(0, above)
        v, vm, vp = window(2, here), window(2, below), window(2, above)
        w = 0.5 * (v + vp)
        flux = w * jnp.where(w > 0, d, dp)
        w = 0.5 * (vm + v)
        flux_below = w * jnp.where(w > 0, dm, d)
        dens_ref[i] = d - courant * (flux - flux_below)
        vrad_ref[i] = window(1, here)
        vphi_ref[i] = v
        return 0

    lax.fori_loop(0, rows, row, 0)


def split(x):
    high = x.astype(bf16)
    return high, (x - high.astype(f32)).astype(bf16)


def split_outside(x):
    high = lax.reduce_precision(x, 8, 7)
    return high.astype(bf16), (x - high).astype(bf16)


def dot3(ah, al, bh, bl):
    def dot(a, b):
        return jnp.dot(a, b, preferred_element_type=f32)

    return dot(ah, bh) + (dot(al, bh) + dot(ah, bl))


def transport(
    edge_ref, d_ref, v_ref, low_ref, high_ref, th_ref, tl_ref, ct_ref, st_ref, out_ref, spec_ref, g_ref
):
    rows, blocks = d_ref.shape[:2]

    def face(da, va, db, vb):
        u = 0.5 * (va + vb)
        return u * jnp.where(u > 0, da, db)

    bottom = jnp.where(edge_ref[0] == 0, face(low_ref[0, 0], low_ref[1, 0], d_ref[0], v_ref[0]), 0.0)
    top = jnp.where(
        edge_ref[1] == 0, face(d_ref[rows - 1], v_ref[rows - 1], high_ref[0, 0], high_ref[1, 0]), 0.0
    )

    def row(i, below):
        flux = face(d_ref[i], v_ref[i], d_ref[i + 1], v_ref[i + 1])
        out_ref[i] = d_ref[i] - courant * (flux - below)
        return flux

    below = lax.fori_loop(0, rows - 1, row, bottom, unroll=4)
    out_ref[rows - 1] = d_ref[rows - 1] - courant * (top - below)

    chunk = 8

    def modes(c, _):
        x = out_ref[pl.ds(c * chunk, chunk)].reshape(chunk * blocks, LANES)
        high, low = split(x)
        g_ref[...] = dot3(high, low, th_ref[...], tl_ref[...])
        for k in range(chunk):
            gc = g_ref[k * blocks : (k + 1) * blocks, :MODES]
            gs = g_ref[k * blocks : (k + 1) * blocks, MODES:]
            ct, st = ct_ref[...], st_ref[...]
            spec_ref[pl.ds(c * chunk + k, 1), :MODES] = jnp.sum(ct * gc - st * gs, 0, keepdims=True)
            spec_ref[pl.ds(c * chunk + k, 1), MODES:] = jnp.sum(st * gc + ct * gs, 0, keepdims=True)
        return 0

    lax.fori_loop(0, rows // chunk, modes, 0)


def embryo_push(
    a_ref, b_ref, r_ref, area_ref, emb_ref, d_ref, cos_ref, sin_ref, hc_ref, hs_ref, x_ref, y_ref, m_ref
):
    rows = d_ref.shape[0]
    count = x_ref.shape[0]

    def weigh(i, _):
        m_ref[i] = d_ref[i] * area_ref[i]
        return 0

    lax.fori_loop(0, rows, weigh, 0, unroll=4)

    def embryo(e, _):
        radius, cos_e, sin_e = emb_ref[e], emb_ref[count + e], emb_ref[2 * count + e]
        cosine, sine = cos_ref[...], sin_ref[...]
        p = gap(emb_ref, e, count, hc_ref, hs_ref)
        base_x, base_y = radius * cos_e, radius * sin_e

        def row(i, sums):
            inverse = lax.rsqrt(a_ref[i * count + e] + b_ref[i * count + e] * p)
            t = inverse * inverse * inverse * m_ref[i]
            return (
                sums[0] + t * (r_ref[i] * cosine - base_x),
                sums[1] + t * (r_ref[i] * sine - base_y),
            )

        zero = jnp.zeros(p.shape, f32)
        x, y = lax.fori_loop(0, rows, row, (zero, zero), unroll=8)
        x_ref[pl.ds(e, 1), :] = jnp.sum(x, 0, keepdims=True)
        y_ref[pl.ds(e, 1), :] = jnp.sum(y, 0, keepdims=True)
        return 0

    lax.fori_loop(0, count, embryo, 0)


def kick(
    r_ref, x_ref, from_ref, rate_ref, ct_ref, st_ref, th_ref, tl_ref, vr_ref, vp_ref, er_ref, ep_ref,
    outr_ref, outp_ref, low_ref, up_ref, zrh_ref, zrl_ref, zph_ref, zpl_ref,
):
    rows, blocks = vr_ref.shape[:2]
    decay, factor = rate_ref[0:1], rate_ref[1:2]
    rweight, aweight = rate_ref[2:3], rate_ref[3:4]

    def sweep(i, carried):
        low, up = carried
        j = rows - 1 - i
        low = x_ref[pl.ds(i, 1), :] + factor * low
        up = x_ref[pl.ds(j, 1), :] + factor * up
        low_ref[pl.ds(i, 1), :] = low
        up_ref[pl.ds(j, 1), :] = up
        return low, up

    lax.fori_loop(0, rows, sweep, (from_ref[0:1], from_ref[1:2]), unroll=4)
    even = decay * (low_ref[...] + up_ref[...] - x_ref[...])
    odd = decay * (low_ref[...] - up_ref[...])
    low_ref[...] = odd * rweight
    up_ref[...] = jnp.concatenate([even[:, MODES:], even[:, :MODES]], axis=1) * aweight

    def twist(i, _):
        ct, st = ct_ref[...], st_ref[...]
        where = pl.ds(pl.multiple_of(i * blocks, blocks), blocks)
        for src, high_ref, low_out in ((low_ref, zrh_ref, zrl_ref), (up_ref, zph_ref, zpl_ref)):
            cc, cs = src[pl.ds(i, 1), :MODES], src[pl.ds(i, 1), MODES:]
            high_ref[where, :MODES], low_out[where, :MODES] = split(cc * ct + cs * st)
            high_ref[where, MODES:], low_out[where, MODES:] = split(cs * ct - cc * st)
        return 0

    lax.fori_loop(0, rows, twist, 0)
    chunk = 8

    def synth(c, _):
        where = pl.ds(pl.multiple_of(c * chunk * blocks, chunk * blocks), chunk * blocks)
        shape = (chunk, blocks, LANES)
        r = dot3(zrh_ref[where], zrl_ref[where], th_ref[...], tl_ref[...]).reshape(shape)
        p = dot3(zph_ref[where], zpl_ref[where], th_ref[...], tl_ref[...]).reshape(shape)
        for k in range(chunk):
            i = c * chunk + k
            scale = gravity / r_ref[i]
            outr_ref[i] = vr_ref[i] + timestep_length * (er_ref[i] + scale * r[k])
            outp_ref[i] = vp_ref[i] + timestep_length * (ep_ref[i] + scale * p[k])
        return 0

    lax.fori_loop(0, rows // chunk, synth, 0)


def butterfly(value, axis):
    count = lax.axis_size(axis)
    step = 1
    while step < count:
        value = value + lax.ppermute(value, axis, [(i, i ^ step) for i in range(count)])
        step *= 2
    return value


def neighbours(block, axis):
    count = lax.axis_size(axis)
    up = [(i, i + 1) for i in range(count - 1)]
    low = lax.ppermute(block[:, -1:], axis, up)
    high = lax.ppermute(block[:, :1], axis, [(t, s) for s, t in up])
    return low, high


def on_device(
    surface_mass,
    outward_drift,
    leftover_angular_drift,
    angular_offsets,
    planetesimal_loop_number,
    planetesimal_angle_bin,
    planetesimal_weights,
):
    rows, sector = surface_mass.shape
    blocks = sector // LANES
    whole = blocks * lax.axis_size("az")
    rad_count = lax.axis_size("rad")
    own = lax.axis_index("rad")
    cycle_first = own * rows
    column_first = lax.axis_index("az") * sector
    cell_step = 2.0 * jnp.pi / ANGULAR_BINS
    embryos = planetesimal_weights.shape[0]
    cube = jax.ShapeDtypeStruct((rows, blocks, LANES), f32)

    piled = jnp.stack([surface_mass, outward_drift, leftover_angular_drift])
    gathered = lax.all_gather(piled.reshape(3, rows, blocks, LANES), "az", axis=2, tiled=True)

    columns = column_first + jnp.arange(sector, dtype=jnp.int32).reshape(blocks, LANES)
    cell_angles = (2 * columns + 1).astype(f32) * (jnp.pi / ANGULAR_BINS)
    cos_cell, sin_cell = jnp.cos(cell_angles), jnp.sin(cell_angles)
    embryo_angles = (2 * planetesimal_angle_bin + 1).astype(f32) * (jnp.pi / ANGULAR_BINS)
    embryo_radii = jnp.exp((planetesimal_loop_number.astype(f32) + 0.5) * cell_step)
    emb = jnp.concatenate(
        [
            embryo_radii,
            jnp.cos(embryo_angles),
            jnp.sin(embryo_angles),
            jnp.cos(0.5 * embryo_angles),
            jnp.sin(0.5 * embryo_angles),
        ]
    )
    half_cos, half_sin = jnp.cos(0.5 * cell_angles), jnp.sin(0.5 * cell_angles)
    cycles = cycle_first + jnp.arange(rows, dtype=jnp.int32)
    radius = jnp.exp((cycles.astype(f32) + 0.5) * cell_step)
    area = radius * radius * cell_step * cell_step
    soften = planetesimal_weights ** (-2.0 / 3.0)
    apart = radius[:, None] - embryo_radii[None]
    a_table = (apart * apart + jnp.square(softening * embryo_radii)[None]) * soften[None]
    b_table = 2.0 * radius[:, None] * soften[None]
    a_table, b_table = a_table.reshape(-1), b_table.reshape(-1)

    orders = jnp.arange(MODES, dtype=jnp.int32)

    def turns(phases):
        angles = (phases % (2 * ANGULAR_BINS)).astype(f32) * (jnp.pi / ANGULAR_BINS)
        return jnp.cos(angles), jnp.sin(angles)

    block_first = column_first + LANES * jnp.arange(blocks, dtype=jnp.int32)
    ct, st = turns((2 * block_first + 1)[:, None] * orders[None])
    lanes = jnp.arange(LANES, dtype=jnp.int32)
    table = jnp.concatenate(turns((2 * lanes)[:, None] * orders[None]), axis=1)
    table_t = jnp.concatenate(turns((2 * lanes)[None] * orders[:, None]), axis=0)
    th, tl = split_outside(table)
    tth, ttl = split_outside(table_t)

    radial_emb, azimuthal_emb = call(
        embryo_field,
        (cube, cube),
        [SMEM] * 4 + [VMEM] * 4,
        [pltpu.VMEM((embryos, blocks, LANES), f32)] * 3,
        flops=600_000_000,
    )(a_table, b_table, radius, emb, cos_cell, sin_cell, half_cos, half_sin)

    start = (column_first - angular_offsets) % ANGULAR_BINS
    dens_two, vrad, vphi = call(
        shift_cycles,
        (cube, cube, cube),
        [SMEM, VMEM],
        [pltpu.VMEM((3, whole + blocks + 8, LANES), f32)],
        flops=10_000_000,
    )(start, gathered)

    low, high = neighbours(jnp.stack([dens_two, vrad]), "rad")
    edges = jnp.stack([own == 0, own == rad_count - 1]).astype(jnp.int32)
    transported, partial = call(
        transport,
        (cube, jax.ShapeDtypeStruct((rows, 2 * MODES), f32)),
        [SMEM] + [VMEM] * 8,
        [pltpu.VMEM((8 * blocks, 2 * MODES), f32)],
        flops=400_000_000,
    )(edges, dens_two, vrad, low, high, th, tl, ct, st)
    line = jax.ShapeDtypeStruct((embryos, LANES), f32)
    push_x, push_y = call(
        embryo_push,
        (line, line),
        [SMEM] * 5 + [VMEM] * 5,
        [pltpu.VMEM((rows, blocks, LANES), f32)],
        flops=600_000_000,
    )(a_table, b_table, radius, area, emb, transported, cos_cell, sin_cell, half_cos, half_sin)
    spectra = butterfly(partial * cell_step, "az")
    push = jnp.stack([jnp.sum(push_x, 1), jnp.sum(push_y, 1)]) / planetesimal_weights[None]
    push = butterfly(butterfly(push, "az"), "rad")

    decays = (jnp.arange(MODES, dtype=f32) + 0.5) * cell_step
    decays = jnp.concatenate([decays, decays])
    local = jnp.arange(rows, dtype=f32)
    rise = jnp.exp(-decays[None] * (rows - 1 - local)[:, None])
    fall = jnp.exp(-decays[None] * local[:, None])
    moments = jnp.stack([jnp.sum(rise * spectra, 0), jnp.sum(fall * spectra, 0)])[None]
    every = lax.all_gather(moments, "rad", axis=0, tiled=True)
    others = jnp.arange(rad_count, dtype=jnp.int32)
    gaps = jnp.stack([own - 1 - others, others - own - 1], axis=1)
    weight = jnp.where(
        gaps[:, :, None] >= 0,
        jnp.exp(-(decays * rows) * jnp.maximum(gaps, 0).astype(f32)[:, :, None]),
        0.0,
    )
    carried = jnp.sum(weight * every, 0)
    doubled = jnp.where(orders > 0, 2.0, 1.0).astype(f32)
    radial_weight = jnp.concatenate([doubled, doubled]) * decays * (-1.0 / cell_step)
    azim_weight = jnp.concatenate([doubled * orders, -doubled * orders])
    rates = jnp.stack([decays, jnp.exp(-decays), radial_weight, azim_weight])
    long = rows * blocks
    kicked_r, kicked_p = call(
        kick,
        (cube, cube),
        [SMEM] + [VMEM] * 11,
        [pltpu.VMEM((rows, 2 * MODES), f32)] * 2 + [pltpu.VMEM((long, 2 * MODES), bf16)] * 4,
        flops=400_000_000,
    )(
        radius, spectra, carried, rates, ct, st, tth, ttl, vrad, vphi, radial_emb, azimuthal_emb
    )
    return (
        transported.reshape(rows, sector),
        kicked_r.reshape(rows, sector),
        kicked_p.reshape(rows, sector),
        push,
    )


def solution(mesh):
    placed = (P("rad", "az"), P("rad", "az"), P("rad", "az"), P("rad"), P(), P(), P())
    return jax.shard_map(
        on_device,
        mesh=mesh,
        in_specs=placed,
        out_specs=(P("rad", "az"), P("rad", "az"), P("rad", "az"), P()),
        check_vma=False,
    )
```

```python
import jax
import jax.numpy as jnp
from jax import lax
from jax.experimental import pallas as pl
from jax.experimental.pallas import tpu as pltpu
from jax.sharding import PartitionSpec as P

ANGULAR_BINS = 16384
MODES = 256
LANES = 128

gravity = 1.0
timestep_length = 0.05
courant = 0.4
softening = 0.02

VMEM = pl.BlockSpec(memory_space=pltpu.VMEM)
SMEM = pl.BlockSpec(memory_space=pltpu.SMEM)
f32 = jnp.float32
bf16 = jnp.bfloat16


def call(body, outs, specs, scratch=(), flops=0):
    return pl.pallas_call(
        body,
        out_shape=outs,
        in_specs=specs,
        out_specs=jax.tree.map(lambda _: VMEM, outs),
        scratch_shapes=list(scratch),
        compiler_params=pltpu.CompilerParams(vmem_limit_bytes=48 * 1024 * 1024),
        cost_estimate=pl.CostEstimate(flops=flops, bytes_accessed=1 << 20, transcendentals=0),
    )


def gap(emb_ref, e, count, half_cos_ref, half_sin_ref):
    s = half_sin_ref[...] * emb_ref[3 * count + e] - half_cos_ref[...] * emb_ref[4 * count + e]
    return 2.0 * emb_ref[e] * (s * s)


def embryo_field(
    a_ref, b_ref, r_ref, emb_ref, cos_ref, sin_ref, hc_ref, hs_ref, rad_ref, azi_ref, p_ref, q_ref, k_ref
):
    count = p_ref.shape[0]

    def prepare(e, _):
        radius, cos_e, sin_e = emb_ref[e], emb_ref[count + e], emb_ref[2 * count + e]
        p_ref[e] = radius * (cos_ref[...] * cos_e + sin_ref[...] * sin_e)
        q_ref[e] = radius * (sin_ref[...] * cos_e - cos_ref[...] * sin_e)
        k_ref[e] = gap(emb_ref, e, count, hc_ref, hs_ref)
        return 0

    lax.fori_loop(0, count, prepare, 0)

    def row(i, _):
        def one(e, sums):
            s0, s1, s2 = sums
            p, q = p_ref[e], q_ref[e]
            inverse = lax.rsqrt(a_ref[i * count + e] + b_ref[i * count + e] * k_ref[e])
            t = inverse * inverse * inverse
            return s0 + t, s1 + t * p, s2 + t * q

        zero = jnp.zeros(p_ref.shape[1:], f32)
        s0, s1, s2 = lax.fori_loop(0, count, one, (zero, zero, zero), unroll=8)
        rad_ref[i] = s1 - r_ref[i] * s0
        azi_ref[i] = -s2
        return 0

    lax.fori_loop(0, rad_ref.shape[0], row, 0)


def ring_gather(own_ref, out_ref, keep_sem, send_sem, recv_sem):
    me = lax.axis_index("az")
    right, left = (me + 1) % 4, (me + 3) % 4
    half = own_ref.shape[1] // 2
    barrier = pltpu.get_barrier_semaphore()
    for peer in (left, right):
        pl.semaphore_signal(
            barrier, inc=1, device_id={"az": peer}, device_id_type=pl.DeviceIdType.MESH
        )
    pl.semaphore_wait(barrier, 2)

    def copy(k, source, slot, part, peer):
        rows = pl.ds(part * half, half)
        return pltpu.make_async_remote_copy(
            src_ref=source.at[:, rows],
            dst_ref=out_ref.at[slot, :, rows],
            send_sem=send_sem.at[k],
            recv_sem=recv_sem.at[k],
            device_id={"az": peer},
            device_id_type=pl.DeviceIdType.MESH,
        )

    firsts = [
        copy(0, own_ref, me, 0, right),
        copy(1, own_ref, me, 1, left),
        copy(2, own_ref, me, 1, right),
        copy(3, own_ref, me, 0, left),
    ]
    for c in firsts:
        c.start()
    keep = pltpu.make_async_copy(own_ref, out_ref.at[me], keep_sem)
    keep.start()
    firsts[0].wait_recv()
    onward = copy(4, out_ref.at[left], left, 0, right)
    onward.start()
    firsts[1].wait_recv()
    back = copy(5, out_ref.at[right], right, 1, left)
    back.start()
    firsts[2].wait_recv()
    firsts[3].wait_recv()
    onward.wait_recv()
    back.wait_recv()
    for c in firsts + [onward, back]:
        c.wait_send()
    keep.wait()


def gather_sectors(piled):
    count = lax.axis_size("az")
    if count != 4:
        return lax.all_gather(piled, "az", axis=0)
    return pl.pallas_call(
        ring_gather,
        out_shape=jax.ShapeDtypeStruct((count,) + piled.shape, f32),
        in_specs=[VMEM],
        out_specs=VMEM,
        scratch_shapes=[
            pltpu.SemaphoreType.DMA,
            pltpu.SemaphoreType.DMA((6,)),
            pltpu.SemaphoreType.DMA((6,)),
        ],
        compiler_params=pltpu.CompilerParams(
            collective_id=0, has_side_effects=True, vmem_limit_bytes=48 * 1024 * 1024
        ),
    )(piled)


def shift_cycles(start_ref, g_ref, dens_ref, vrad_ref, vphi_ref, line_ref):
    rows, blocks = dens_ref.shape[:2]
    sectors = g_ref.shape[0]
    whole = sectors * blocks
    total = whole * LANES
    extra = line_ref.shape[1] - whole
    lane = lax.broadcasted_iota(jnp.int32, (blocks, LANES), 1)

    def window(field, start):
        block = start // LANES
        rest = start % LANES
        first = pltpu.roll(line_ref[field, pl.ds(block, blocks), :], LANES - rest, 1)
        second = pltpu.roll(line_ref[field, pl.ds(block + 1, blocks), :], LANES - rest, 1)
        return jnp.where(lane < LANES - rest, first, second)

    def row(i, _):
        for field in range(3):
            for k in range(sectors):
                line_ref[field, k * blocks : (k + 1) * blocks] = g_ref[k, field, i]
            line_ref[field, whole : whole + blocks] = g_ref[0, field, i]
            line_ref[field, whole + blocks :] = g_ref[1 % sectors, field, i, : extra - blocks]
        here = start_ref[i]
        below = (here + total - 1) % total
        above = (here + 1) % total
        d, dm, dp = window(0, here), window(0, below), window(0, above)
        v, vm, vp = window(2, here), window(2, below), window(2, above)
        w = 0.5 * (v + vp)
        flux = w * jnp.where(w > 0, d, dp)
        w = 0.5 * (vm + v)
        flux_below = w * jnp.where(w > 0, dm, d)
        dens_ref[i] = d - courant * (flux - flux_below)
        vrad_ref[i] = window(1, here)
        vphi_ref[i] = v
        return 0

    lax.fori_loop(0, rows, row, 0)


def split(x):
    high = x.astype(bf16)
    return high, (x - high.astype(f32)).astype(bf16)


def split_outside(x):
    high = lax.reduce_precision(x, 8, 7)
    return high.astype(bf16), (x - high).astype(bf16)


def dot3(ah, al, bh, bl):
    def dot(a, b):
        return jnp.dot(a, b, preferred_element_type=f32)

    return dot(ah, bh) + (dot(al, bh) + dot(ah, bl))


def transport(
    edge_ref, d_ref, v_ref, low_ref, high_ref, th_ref, tl_ref, ct_ref, st_ref, out_ref, spec_ref, g_ref
):
    rows, blocks = d_ref.shape[:2]

    def face(da, va, db, vb):
        u = 0.5 * (va + vb)
        return u * jnp.where(u > 0, da, db)

    bottom = jnp.where(edge_ref[0] == 0, face(low_ref[0, 0], low_ref[1, 0], d_ref[0], v_ref[0]), 0.0)
    top = jnp.where(
        edge_ref[1] == 0, face(d_ref[rows - 1], v_ref[rows - 1], high_ref[0, 0], high_ref[1, 0]), 0.0
    )

    def row(i, below):
        flux = face(d_ref[i], v_ref[i], d_ref[i + 1], v_ref[i + 1])
        out_ref[i] = d_ref[i] - courant * (flux - below)
        return flux

    below = lax.fori_loop(0, rows - 1, row, bottom, unroll=4)
    out_ref[rows - 1] = d_ref[rows - 1] - courant * (top - below)

    chunk = 8

    def modes(c, _):
        x = out_ref[pl.ds(c * chunk, chunk)].reshape(chunk * blocks, LANES)
        high, low = split(x)
        g_ref[...] = dot3(high, low, th_ref[...], tl_ref[...])
        for k in range(chunk):
            gc = g_ref[k * blocks : (k + 1) * blocks, :MODES]
            gs = g_ref[k * blocks : (k + 1) * blocks, MODES:]
            ct, st = ct_ref[...], st_ref[...]
            spec_ref[pl.ds(c * chunk + k, 1), :MODES] = jnp.sum(ct * gc - st * gs, 0, keepdims=True)
            spec_ref[pl.ds(c * chunk + k, 1), MODES:] = jnp.sum(st * gc + ct * gs, 0, keepdims=True)
        return 0

    lax.fori_loop(0, rows // chunk, modes, 0)


def embryo_push(
    a_ref, b_ref, r_ref, area_ref, emb_ref, d_ref, cos_ref, sin_ref, hc_ref, hs_ref, x_ref, y_ref, m_ref
):
    rows = d_ref.shape[0]
    count = x_ref.shape[0]

    def weigh(i, _):
        m_ref[i] = d_ref[i] * area_ref[i]
        return 0

    lax.fori_loop(0, rows, weigh, 0, unroll=4)

    def embryo(e, _):
        radius, cos_e, sin_e = emb_ref[e], emb_ref[count + e], emb_ref[2 * count + e]
        cosine, sine = cos_ref[...], sin_ref[...]
        p = gap(emb_ref, e, count, hc_ref, hs_ref)
        base_x, base_y = radius * cos_e, radius * sin_e

        def row(i, sums):
            inverse = lax.rsqrt(a_ref[i * count + e] + b_ref[i * count + e] * p)
            t = inverse * inverse * inverse * m_ref[i]
            return (
                sums[0] + t * (r_ref[i] * cosine - base_x),
                sums[1] + t * (r_ref[i] * sine - base_y),
            )

        zero = jnp.zeros(p.shape, f32)
        x, y = lax.fori_loop(0, rows, row, (zero, zero), unroll=8)
        x_ref[pl.ds(e, 1), :] = jnp.sum(x, 0, keepdims=True)
        y_ref[pl.ds(e, 1), :] = jnp.sum(y, 0, keepdims=True)
        return 0

    lax.fori_loop(0, count, embryo, 0)


def kick(
    r_ref, x_ref, from_ref, rate_ref, ct_ref, st_ref, th_ref, tl_ref, vr_ref, vp_ref, er_ref, ep_ref,
    outr_ref, outp_ref, low_ref, up_ref, zrh_ref, zrl_ref, zph_ref, zpl_ref,
):
    rows, blocks = vr_ref.shape[:2]
    decay, factor = rate_ref[0:1], rate_ref[1:2]
    rweight, aweight = rate_ref[2:3], rate_ref[3:4]

    def sweep(i, carried):
        low, up = carried
        j = rows - 1 - i
        low = x_ref[pl.ds(i, 1), :] + factor * low
        up = x_ref[pl.ds(j, 1), :] + factor * up
        low_ref[pl.ds(i, 1), :] = low
        up_ref[pl.ds(j, 1), :] = up
        return low, up

    lax.fori_loop(0, rows, sweep, (from_ref[0:1], from_ref[1:2]), unroll=4)
    even = decay * (low_ref[...] + up_ref[...] - x_ref[...])
    odd = decay * (low_ref[...] - up_ref[...])
    low_ref[...] = odd * rweight
    up_ref[...] = jnp.concatenate([even[:, MODES:], even[:, :MODES]], axis=1) * aweight

    def twist(i, _):
        ct, st = ct_ref[...], st_ref[...]
        where = pl.ds(pl.multiple_of(i * blocks, blocks), blocks)
        for src, high_ref, low_out in ((low_ref, zrh_ref, zrl_ref), (up_ref, zph_ref, zpl_ref)):
            cc, cs = src[pl.ds(i, 1), :MODES], src[pl.ds(i, 1), MODES:]
            high_ref[where, :MODES], low_out[where, :MODES] = split(cc * ct + cs * st)
            high_ref[where, MODES:], low_out[where, MODES:] = split(cs * ct - cc * st)
        return 0

    lax.fori_loop(0, rows, twist, 0)
    chunk = 8

    def synth(c, _):
        where = pl.ds(pl.multiple_of(c * chunk * blocks, chunk * blocks), chunk * blocks)
        shape = (chunk, blocks, LANES)
        r = dot3(zrh_ref[where], zrl_ref[where], th_ref[...], tl_ref[...]).reshape(shape)
        p = dot3(zph_ref[where], zpl_ref[where], th_ref[...], tl_ref[...]).reshape(shape)
        for k in range(chunk):
            i = c * chunk + k
            scale = gravity / r_ref[i]
            outr_ref[i] = vr_ref[i] + timestep_length * (er_ref[i] + scale * r[k])
            outp_ref[i] = vp_ref[i] + timestep_length * (ep_ref[i] + scale * p[k])
        return 0

    lax.fori_loop(0, rows // chunk, synth, 0)


def butterfly(value, axis):
    count = lax.axis_size(axis)
    step = 1
    while step < count:
        value = value + lax.ppermute(value, axis, [(i, i ^ step) for i in range(count)])
        step *= 2
    return value


def neighbours(block, axis):
    count = lax.axis_size(axis)
    up = [(i, i + 1) for i in range(count - 1)]
    low = lax.ppermute(block[:, -1:], axis, up)
    high = lax.ppermute(block[:, :1], axis, [(t, s) for s, t in up])
    return low, high


def on_device(
    surface_mass,
    outward_drift,
    leftover_angular_drift,
    angular_offsets,
    planetesimal_loop_number,
    planetesimal_angle_bin,
    planetesimal_weights,
):
    rows, sector = surface_mass.shape
    blocks = sector // LANES
    whole = blocks * lax.axis_size("az")
    rad_count = lax.axis_size("rad")
    own = lax.axis_index("rad")
    cycle_first = own * rows
    column_first = lax.axis_index("az") * sector
    cell_step = 2.0 * jnp.pi / ANGULAR_BINS
    embryos = planetesimal_weights.shape[0]
    cube = jax.ShapeDtypeStruct((rows, blocks, LANES), f32)

    piled = jnp.stack([surface_mass, outward_drift, leftover_angular_drift])
    gathered = gather_sectors(piled.reshape(3, rows, blocks, LANES))

    columns = column_first + jnp.arange(sector, dtype=jnp.int32).reshape(blocks, LANES)
    cell_angles = (2 * columns + 1).astype(f32) * (jnp.pi / ANGULAR_BINS)
    cos_cell, sin_cell = jnp.cos(cell_angles), jnp.sin(cell_angles)
    embryo_angles = (2 * planetesimal_angle_bin + 1).astype(f32) * (jnp.pi / ANGULAR_BINS)
    embryo_radii = jnp.exp((planetesimal_loop_number.astype(f32) + 0.5) * cell_step)
    emb = jnp.concatenate(
        [
            embryo_radii,
            jnp.cos(embryo_angles),
            jnp.sin(embryo_angles),
            jnp.cos(0.5 * embryo_angles),
            jnp.sin(0.5 * embryo_angles),
        ]
    )
    half_cos, half_sin = jnp.cos(0.5 * cell_angles), jnp.sin(0.5 * cell_angles)
    cycles = cycle_first + jnp.arange(rows, dtype=jnp.int32)
    radius = jnp.exp((cycles.astype(f32) + 0.5) * cell_step)
    area = radius * radius * cell_step * cell_step
    soften = planetesimal_weights ** (-2.0 / 3.0)
    apart = radius[:, None] - embryo_radii[None]
    a_table = (apart * apart + jnp.square(softening * embryo_radii)[None]) * soften[None]
    b_table = 2.0 * radius[:, None] * soften[None]
    a_table, b_table = a_table.reshape(-1), b_table.reshape(-1)

    orders = jnp.arange(MODES, dtype=jnp.int32)

    def turns(phases):
        angles = (phases % (2 * ANGULAR_BINS)).astype(f32) * (jnp.pi / ANGULAR_BINS)
        return jnp.cos(angles), jnp.sin(angles)

    block_first = column_first + LANES * jnp.arange(blocks, dtype=jnp.int32)
    ct, st = turns((2 * block_first + 1)[:, None] * orders[None])
    lanes = jnp.arange(LANES, dtype=jnp.int32)
    table = jnp.concatenate(turns((2 * lanes)[:, None] * orders[None]), axis=1)
    table_t = jnp.concatenate(turns((2 * lanes)[None] * orders[:, None]), axis=0)
    th, tl = split_outside(table)
    tth, ttl = split_outside(table_t)

    radial_emb, azimuthal_emb = call(
        embryo_field,
        (cube, cube),
        [SMEM] * 4 + [VMEM] * 4,
        [pltpu.VMEM((embryos, blocks, LANES), f32)] * 3,
        flops=600_000_000,
    )(a_table, b_table, radius, emb, cos_cell, sin_cell, half_cos, half_sin)

    start = (column_first - angular_offsets) % ANGULAR_BINS
    dens_two, vrad, vphi = call(
        shift_cycles,
        (cube, cube, cube),
        [SMEM, VMEM],
        [pltpu.VMEM((3, whole + blocks + 8, LANES), f32)],
        flops=10_000_000,
    )(start, gathered)

    low, high = neighbours(jnp.stack([dens_two, vrad]), "rad")
    edges = jnp.stack([own == 0, own == rad_count - 1]).astype(jnp.int32)
    transported, partial = call(
        transport,
        (cube, jax.ShapeDtypeStruct((rows, 2 * MODES), f32)),
        [SMEM] + [VMEM] * 8,
        [pltpu.VMEM((8 * blocks, 2 * MODES), f32)],
        flops=400_000_000,
    )(edges, dens_two, vrad, low, high, th, tl, ct, st)
    line = jax.ShapeDtypeStruct((embryos, LANES), f32)
    push_x, push_y = call(
        embryo_push,
        (line, line),
        [SMEM] * 5 + [VMEM] * 5,
        [pltpu.VMEM((rows, blocks, LANES), f32)],
        flops=600_000_000,
    )(a_table, b_table, radius, area, emb, transported, cos_cell, sin_cell, half_cos, half_sin)
    spectra = butterfly(partial * cell_step, "az")
    push = jnp.stack([jnp.sum(push_x, 1), jnp.sum(push_y, 1)]) / planetesimal_weights[None]
    push = butterfly(butterfly(push, "az"), "rad")

    decays = (jnp.arange(MODES, dtype=f32) + 0.5) * cell_step
    decays = jnp.concatenate([decays, decays])
    local = jnp.arange(rows, dtype=f32)
    rise = jnp.exp(-decays[None] * (rows - 1 - local)[:, None])
    fall = jnp.exp(-decays[None] * local[:, None])
    moments = jnp.stack([jnp.sum(rise * spectra, 0), jnp.sum(fall * spectra, 0)])[None]
    every = lax.all_gather(moments, "rad", axis=0, tiled=True)
    others = jnp.arange(rad_count, dtype=jnp.int32)
    gaps = jnp.stack([own - 1 - others, others - own - 1], axis=1)
    weight = jnp.where(
        gaps[:, :, None] >= 0,
        jnp.exp(-(decays * rows) * jnp.maximum(gaps, 0).astype(f32)[:, :, None]),
        0.0,
    )
    carried = jnp.sum(weight * every, 0)
    doubled = jnp.where(orders > 0, 2.0, 1.0).astype(f32)
    radial_weight = jnp.concatenate([doubled, doubled]) * decays * (-1.0 / cell_step)
    azim_weight = jnp.concatenate([doubled * orders, -doubled * orders])
    rates = jnp.stack([decays, jnp.exp(-decays), radial_weight, azim_weight])
    long = rows * blocks
    kicked_r, kicked_p = call(
        kick,
        (cube, cube),
        [SMEM] + [VMEM] * 11,
        [pltpu.VMEM((rows, 2 * MODES), f32)] * 2 + [pltpu.VMEM((long, 2 * MODES), bf16)] * 4,
        flops=400_000_000,
    )(
        radius, spectra, carried, rates, ct, st, tth, ttl, vrad, vphi, radial_emb, azimuthal_emb
    )
    return (
        transported.reshape(rows, sector),
        kicked_r.reshape(rows, sector),
        kicked_p.reshape(rows, sector),
        push,
    )


def solution(mesh):
    placed = (P("rad", "az"), P("rad", "az"), P("rad", "az"), P("rad"), P(), P(), P())
    return jax.shard_map(
        on_device,
        mesh=mesh,
        in_specs=placed,
        out_specs=(P("rad", "az"), P("rad", "az"), P("rad", "az"), P()),
        check_vma=False,
    )
```

```python
import jax
import jax.numpy as jnp
from jax import lax
from jax.experimental import pallas as pl
from jax.experimental.pallas import tpu as pltpu
from jax.sharding import PartitionSpec as P

ANGULAR_BINS = 16384
MODES = 256
LANES = 128

gravity = 1.0
timestep_length = 0.05
courant = 0.4
softening = 0.02

VMEM = pl.BlockSpec(memory_space=pltpu.VMEM)
SMEM = pl.BlockSpec(memory_space=pltpu.SMEM)
f32 = jnp.float32
bf16 = jnp.bfloat16


def call(body, outs, specs, scratch=(), flops=0):
    return pl.pallas_call(
        body,
        out_shape=outs,
        in_specs=specs,
        out_specs=jax.tree.map(lambda _: VMEM, outs),
        scratch_shapes=list(scratch),
        compiler_params=pltpu.CompilerParams(vmem_limit_bytes=48 * 1024 * 1024),
        cost_estimate=pl.CostEstimate(flops=flops, bytes_accessed=1 << 20, transcendentals=0),
    )


def gap(emb_ref, e, count, half_cos_ref, half_sin_ref):
    s = half_sin_ref[...] * emb_ref[3 * count + e] - half_cos_ref[...] * emb_ref[4 * count + e]
    return 2.0 * emb_ref[e] * (s * s)


def embryo_field(
    a_ref, b_ref, r_ref, emb_ref, cos_ref, sin_ref, hc_ref, hs_ref, rad_ref, azi_ref, p_ref, q_ref, k_ref
):
    count = p_ref.shape[0]

    def prepare(e, _):
        radius, cos_e, sin_e = emb_ref[e], emb_ref[count + e], emb_ref[2 * count + e]
        p_ref[e] = radius * (cos_ref[...] * cos_e + sin_ref[...] * sin_e)
        q_ref[e] = radius * (sin_ref[...] * cos_e - cos_ref[...] * sin_e)
        k_ref[e] = gap(emb_ref, e, count, hc_ref, hs_ref)
        return 0

    lax.fori_loop(0, count, prepare, 0)

    def row(i, _):
        def one(e, sums):
            s0, s1, s2 = sums
            p, q = p_ref[e], q_ref[e]
            inverse = lax.rsqrt(a_ref[i * count + e] + b_ref[i * count + e] * k_ref[e])
            t = inverse * inverse * inverse
            return s0 + t, s1 + t * p, s2 + t * q

        zero = jnp.zeros(p_ref.shape[1:], f32)
        s0, s1, s2 = lax.fori_loop(0, count, one, (zero, zero, zero), unroll=8)
        rad_ref[i] = s1 - r_ref[i] * s0
        azi_ref[i] = -s2
        return 0

    lax.fori_loop(0, rad_ref.shape[0], row, 0)


def ring_gather(own_ref, *refs):
    *field_refs, keep_sem, send_sem, recv_sem = refs
    out_ref = field_refs.pop(8)
    me = lax.axis_index("az")
    right, left = (me + 1) % 4, (me + 3) % 4
    half = own_ref.shape[1] // 2
    barrier = pltpu.get_barrier_semaphore()
    for peer in (left, right):
        pl.semaphore_signal(
            barrier, inc=1, device_id={"az": peer}, device_id_type=pl.DeviceIdType.MESH
        )
    pl.semaphore_wait(barrier, 2)

    def copy(k, source, slot, part, peer):
        rows = pl.ds(part * half, half)
        return pltpu.make_async_remote_copy(
            src_ref=source.at[:, rows],
            dst_ref=out_ref.at[slot, :, rows],
            send_sem=send_sem.at[k],
            recv_sem=recv_sem.at[k],
            device_id={"az": peer},
            device_id_type=pl.DeviceIdType.MESH,
        )

    firsts = [
        copy(0, own_ref, me, 0, right),
        copy(1, own_ref, me, 1, left),
        copy(2, own_ref, me, 1, right),
        copy(3, own_ref, me, 0, left),
    ]
    for c in firsts:
        c.start()
    keep = pltpu.make_async_copy(own_ref, out_ref.at[me], keep_sem)
    keep.start()
    embryo_field(*field_refs)
    firsts[0].wait_recv()
    onward = copy(4, out_ref.at[left], left, 0, right)
    onward.start()
    firsts[1].wait_recv()
    back = copy(5, out_ref.at[right], right, 1, left)
    back.start()
    firsts[2].wait_recv()
    firsts[3].wait_recv()
    onward.wait_recv()
    back.wait_recv()
    for c in firsts + [onward, back]:
        c.wait_send()
    keep.wait()


def gather_sectors(piled, tables, embryos):
    count = lax.axis_size("az")
    cube = jax.ShapeDtypeStruct(piled.shape[1:], f32)
    scratch = [pltpu.VMEM((embryos,) + piled.shape[2:], f32)] * 3
    if count != 4:
        fields = call(
            embryo_field, (cube, cube), [SMEM] * 4 + [VMEM] * 4, scratch, flops=600_000_000
        )(*tables)
        return (lax.all_gather(piled, "az", axis=0),) + tuple(fields)
    return pl.pallas_call(
        ring_gather,
        out_shape=(jax.ShapeDtypeStruct((count,) + piled.shape, f32), cube, cube),
        in_specs=[VMEM] + [SMEM] * 4 + [VMEM] * 4,
        out_specs=(VMEM,) * 3,
        scratch_shapes=[
            *scratch,
            pltpu.SemaphoreType.DMA,
            pltpu.SemaphoreType.DMA((6,)),
            pltpu.SemaphoreType.DMA((6,)),
        ],
        compiler_params=pltpu.CompilerParams(
            collective_id=0, has_side_effects=True, vmem_limit_bytes=48 * 1024 * 1024
        ),
    )(piled, *tables)


def shift_cycles(start_ref, g_ref, dens_ref, vrad_ref, vphi_ref, line_ref):
    rows, blocks = dens_ref.shape[:2]
    sectors = g_ref.shape[0]
    whole = sectors * blocks
    total = whole * LANES
    extra = line_ref.shape[1] - whole
    lane = lax.broadcasted_iota(jnp.int32, (blocks, LANES), 1)

    def window(field, start):
        block = start // LANES
        rest = start % LANES
        first = pltpu.roll(line_ref[field, pl.ds(block, blocks), :], LANES - rest, 1)
        second = pltpu.roll(line_ref[field, pl.ds(block + 1, blocks), :], LANES - rest, 1)
        return jnp.where(lane < LANES - rest, first, second)

    def row(i, _):
        for field in range(3):
            for k in range(sectors):
                line_ref[field, k * blocks : (k + 1) * blocks] = g_ref[k, field, i]
            line_ref[field, whole : whole + blocks] = g_ref[0, field, i]
            line_ref[field, whole + blocks :] = g_ref[1 % sectors, field, i, : extra - blocks]
        here = start_ref[i]
        below = (here + total - 1) % total
        above = (here + 1) % total
        d, dm, dp = window(0, here), window(0, below), window(0, above)
        v, vm, vp = window(2, here), window(2, below), window(2, above)
        w = 0.5 * (v + vp)
        flux = w * jnp.where(w > 0, d, dp)
        w = 0.5 * (vm + v)
        flux_below = w * jnp.where(w > 0, dm, d)
        dens_ref[i] = d - courant * (flux - flux_below)
        vrad_ref[i] = window(1, here)
        vphi_ref[i] = v
        return 0

    lax.fori_loop(0, rows, row, 0)


def split(x):
    high = x.astype(bf16)
    return high, (x - high.astype(f32)).astype(bf16)


def split_outside(x):
    high = lax.reduce_precision(x, 8, 7)
    return high.astype(bf16), (x - high).astype(bf16)


def dot3(ah, al, bh, bl):
    def dot(a, b):
        return jnp.dot(a, b, preferred_element_type=f32)

    return dot(ah, bh) + (dot(al, bh) + dot(ah, bl))


def transport(
    edge_ref, d_ref, v_ref, low_ref, high_ref, th_ref, tl_ref, ct_ref, st_ref, out_ref, spec_ref, g_ref
):
    rows, blocks = d_ref.shape[:2]

    def face(da, va, db, vb):
        u = 0.5 * (va + vb)
        return u * jnp.where(u > 0, da, db)

    bottom = jnp.where(edge_ref[0] == 0, face(low_ref[0, 0], low_ref[1, 0], d_ref[0], v_ref[0]), 0.0)
    top = jnp.where(
        edge_ref[1] == 0, face(d_ref[rows - 1], v_ref[rows - 1], high_ref[0, 0], high_ref[1, 0]), 0.0
    )

    def row(i, below):
        flux = face(d_ref[i], v_ref[i], d_ref[i + 1], v_ref[i + 1])
        out_ref[i] = d_ref[i] - courant * (flux - below)
        return flux

    below = lax.fori_loop(0, rows - 1, row, bottom, unroll=4)
    out_ref[rows - 1] = d_ref[rows - 1] - courant * (top - below)

    chunk = 8

    def modes(c, _):
        x = out_ref[pl.ds(c * chunk, chunk)].reshape(chunk * blocks, LANES)
        high, low = split(x)
        g_ref[...] = dot3(high, low, th_ref[...], tl_ref[...])
        for k in range(chunk):
            gc = g_ref[k * blocks : (k + 1) * blocks, :MODES]
            gs = g_ref[k * blocks : (k + 1) * blocks, MODES:]
            ct, st = ct_ref[...], st_ref[...]
            spec_ref[pl.ds(c * chunk + k, 1), :MODES] = jnp.sum(ct * gc - st * gs, 0, keepdims=True)
            spec_ref[pl.ds(c * chunk + k, 1), MODES:] = jnp.sum(st * gc + ct * gs, 0, keepdims=True)
        return 0

    lax.fori_loop(0, rows // chunk, modes, 0)


def embryo_push(
    a_ref, b_ref, r_ref, area_ref, emb_ref, d_ref, cos_ref, sin_ref, hc_ref, hs_ref, x_ref, y_ref, m_ref
):
    rows = d_ref.shape[0]
    count = x_ref.shape[0]

    def weigh(i, _):
        m_ref[i] = d_ref[i] * area_ref[i]
        return 0

    lax.fori_loop(0, rows, weigh, 0, unroll=4)

    def embryo(e, _):
        radius, cos_e, sin_e = emb_ref[e], emb_ref[count + e], emb_ref[2 * count + e]
        cosine, sine = cos_ref[...], sin_ref[...]
        p = gap(emb_ref, e, count, hc_ref, hs_ref)
        base_x, base_y = radius * cos_e, radius * sin_e

        def row(i, sums):
            inverse = lax.rsqrt(a_ref[i * count + e] + b_ref[i * count + e] * p)
            t = inverse * inverse * inverse * m_ref[i]
            return (
                sums[0] + t * (r_ref[i] * cosine - base_x),
                sums[1] + t * (r_ref[i] * sine - base_y),
            )

        zero = jnp.zeros(p.shape, f32)
        x, y = lax.fori_loop(0, rows, row, (zero, zero), unroll=8)
        x_ref[pl.ds(e, 1), :] = jnp.sum(x, 0, keepdims=True)
        y_ref[pl.ds(e, 1), :] = jnp.sum(y, 0, keepdims=True)
        return 0

    lax.fori_loop(0, count, embryo, 0)


def kick(
    r_ref, x_ref, from_ref, rate_ref, ct_ref, st_ref, th_ref, tl_ref, vr_ref, vp_ref, er_ref, ep_ref,
    outr_ref, outp_ref, low_ref, up_ref, zrh_ref, zrl_ref, zph_ref, zpl_ref,
):
    rows, blocks = vr_ref.shape[:2]
    decay, factor = rate_ref[0:1], rate_ref[1:2]
    rweight, aweight = rate_ref[2:3], rate_ref[3:4]

    def sweep(i, carried):
        low, up = carried
        j = rows - 1 - i
        low = x_ref[pl.ds(i, 1), :] + factor * low
        up = x_ref[pl.ds(j, 1), :] + factor * up
        low_ref[pl.ds(i, 1), :] = low
        up_ref[pl.ds(j, 1), :] = up
        return low, up

    lax.fori_loop(0, rows, sweep, (from_ref[0:1], from_ref[1:2]), unroll=4)
    even = decay * (low_ref[...] + up_ref[...] - x_ref[...])
    odd = decay * (low_ref[...] - up_ref[...])
    low_ref[...] = odd * rweight
    up_ref[...] = jnp.concatenate([even[:, MODES:], even[:, :MODES]], axis=1) * aweight

    def twist(i, _):
        ct, st = ct_ref[...], st_ref[...]
        where = pl.ds(pl.multiple_of(i * blocks, blocks), blocks)
        for src, high_ref, low_out in ((low_ref, zrh_ref, zrl_ref), (up_ref, zph_ref, zpl_ref)):
            cc, cs = src[pl.ds(i, 1), :MODES], src[pl.ds(i, 1), MODES:]
            high_ref[where, :MODES], low_out[where, :MODES] = split(cc * ct + cs * st)
            high_ref[where, MODES:], low_out[where, MODES:] = split(cs * ct - cc * st)
        return 0

    lax.fori_loop(0, rows, twist, 0)
    chunk = 8

    def synth(c, _):
        where = pl.ds(pl.multiple_of(c * chunk * blocks, chunk * blocks), chunk * blocks)
        shape = (chunk, blocks, LANES)
        r = dot3(zrh_ref[where], zrl_ref[where], th_ref[...], tl_ref[...]).reshape(shape)
        p = dot3(zph_ref[where], zpl_ref[where], th_ref[...], tl_ref[...]).reshape(shape)
        for k in range(chunk):
            i = c * chunk + k
            scale = gravity / r_ref[i]
            outr_ref[i] = vr_ref[i] + timestep_length * (er_ref[i] + scale * r[k])
            outp_ref[i] = vp_ref[i] + timestep_length * (ep_ref[i] + scale * p[k])
        return 0

    lax.fori_loop(0, rows // chunk, synth, 0)


def butterfly(value, axis):
    count = lax.axis_size(axis)
    step = 1
    while step < count:
        value = value + lax.ppermute(value, axis, [(i, i ^ step) for i in range(count)])
        step *= 2
    return value


def neighbours(block, axis):
    count = lax.axis_size(axis)
    up = [(i, i + 1) for i in range(count - 1)]
    low = lax.ppermute(block[:, -1:], axis, up)
    high = lax.ppermute(block[:, :1], axis, [(t, s) for s, t in up])
    return low, high


def on_device(
    surface_mass,
    outward_drift,
    leftover_angular_drift,
    angular_offsets,
    planetesimal_loop_number,
    planetesimal_angle_bin,
    planetesimal_weights,
):
    rows, sector = surface_mass.shape
    blocks = sector // LANES
    whole = blocks * lax.axis_size("az")
    rad_count = lax.axis_size("rad")
    own = lax.axis_index("rad")
    cycle_first = own * rows
    column_first = lax.axis_index("az") * sector
    cell_step = 2.0 * jnp.pi / ANGULAR_BINS
    embryos = planetesimal_weights.shape[0]
    cube = jax.ShapeDtypeStruct((rows, blocks, LANES), f32)

    piled = jnp.stack([surface_mass, outward_drift, leftover_angular_drift])

    columns = column_first + jnp.arange(sector, dtype=jnp.int32).reshape(blocks, LANES)
    cell_angles = (2 * columns + 1).astype(f32) * (jnp.pi / ANGULAR_BINS)
    cos_cell, sin_cell = jnp.cos(cell_angles), jnp.sin(cell_angles)
    embryo_angles = (2 * planetesimal_angle_bin + 1).astype(f32) * (jnp.pi / ANGULAR_BINS)
    embryo_radii = jnp.exp((planetesimal_loop_number.astype(f32) + 0.5) * cell_step)
    emb = jnp.concatenate(
        [
            embryo_radii,
            jnp.cos(embryo_angles),
            jnp.sin(embryo_angles),
            jnp.cos(0.5 * embryo_angles),
            jnp.sin(0.5 * embryo_angles),
        ]
    )
    half_cos, half_sin = jnp.cos(0.5 * cell_angles), jnp.sin(0.5 * cell_angles)
    cycles = cycle_first + jnp.arange(rows, dtype=jnp.int32)
    radius = jnp.exp((cycles.astype(f32) + 0.5) * cell_step)
    area = radius * radius * cell_step * cell_step
    soften = planetesimal_weights ** (-2.0 / 3.0)
    apart = radius[:, None] - embryo_radii[None]
    a_table = (apart * apart + jnp.square(softening * embryo_radii)[None]) * soften[None]
    b_table = 2.0 * radius[:, None] * soften[None]
    a_table, b_table = a_table.reshape(-1), b_table.reshape(-1)

    orders = jnp.arange(MODES, dtype=jnp.int32)

    def turns(phases):
        angles = (phases % (2 * ANGULAR_BINS)).astype(f32) * (jnp.pi / ANGULAR_BINS)
        return jnp.cos(angles), jnp.sin(angles)

    block_first = column_first + LANES * jnp.arange(blocks, dtype=jnp.int32)
    ct, st = turns((2 * block_first + 1)[:, None] * orders[None])
    lanes = jnp.arange(LANES, dtype=jnp.int32)
    table = jnp.concatenate(turns((2 * lanes)[:, None] * orders[None]), axis=1)
    table_t = jnp.concatenate(turns((2 * lanes)[None] * orders[:, None]), axis=0)
    th, tl = split_outside(table)
    tth, ttl = split_outside(table_t)

    tables = (a_table, b_table, radius, emb, cos_cell, sin_cell, half_cos, half_sin)
    gathered, radial_emb, azimuthal_emb = gather_sectors(
        piled.reshape(3, rows, blocks, LANES), tables, embryos
    )

    start = (column_first - angular_offsets) % ANGULAR_BINS
    dens_two, vrad, vphi = call(
        shift_cycles,
        (cube, cube, cube),
        [SMEM, VMEM],
        [pltpu.VMEM((3, whole + blocks + 8, LANES), f32)],
        flops=10_000_000,
    )(start, gathered)

    low, high = neighbours(jnp.stack([dens_two, vrad]), "rad")
    edges = jnp.stack([own == 0, own == rad_count - 1]).astype(jnp.int32)
    transported, partial = call(
        transport,
        (cube, jax.ShapeDtypeStruct((rows, 2 * MODES), f32)),
        [SMEM] + [VMEM] * 8,
        [pltpu.VMEM((8 * blocks, 2 * MODES), f32)],
        flops=400_000_000,
    )(edges, dens_two, vrad, low, high, th, tl, ct, st)
    line = jax.ShapeDtypeStruct((embryos, LANES), f32)
    push_x, push_y = call(
        embryo_push,
        (line, line),
        [SMEM] * 5 + [VMEM] * 5,
        [pltpu.VMEM((rows, blocks, LANES), f32)],
        flops=600_000_000,
    )(a_table, b_table, radius, area, emb, transported, cos_cell, sin_cell, half_cos, half_sin)
    spectra = butterfly(partial * cell_step, "az")
    push = jnp.stack([jnp.sum(push_x, 1), jnp.sum(push_y, 1)]) / planetesimal_weights[None]
    push = butterfly(butterfly(push, "az"), "rad")

    decays = (jnp.arange(MODES, dtype=f32) + 0.5) * cell_step
    decays = jnp.concatenate([decays, decays])
    local = jnp.arange(rows, dtype=f32)
    rise = jnp.exp(-decays[None] * (rows - 1 - local)[:, None])
    fall = jnp.exp(-decays[None] * local[:, None])
    moments = jnp.stack([jnp.sum(rise * spectra, 0), jnp.sum(fall * spectra, 0)])[None]
    every = lax.all_gather(moments, "rad", axis=0, tiled=True)
    others = jnp.arange(rad_count, dtype=jnp.int32)
    gaps = jnp.stack([own - 1 - others, others - own - 1], axis=1)
    weight = jnp.where(
        gaps[:, :, None] >= 0,
        jnp.exp(-(decays * rows) * jnp.maximum(gaps, 0).astype(f32)[:, :, None]),
        0.0,
    )
    carried = jnp.sum(weight * every, 0)
    doubled = jnp.where(orders > 0, 2.0, 1.0).astype(f32)
    radial_weight = jnp.concatenate([doubled, doubled]) * decays * (-1.0 / cell_step)
    azim_weight = jnp.concatenate([doubled * orders, -doubled * orders])
    rates = jnp.stack([decays, jnp.exp(-decays), radial_weight, azim_weight])
    long = rows * blocks
    kicked_r, kicked_p = call(
        kick,
        (cube, cube),
        [SMEM] + [VMEM] * 11,
        [pltpu.VMEM((rows, 2 * MODES), f32)] * 2 + [pltpu.VMEM((long, 2 * MODES), bf16)] * 4,
        flops=400_000_000,
    )(
        radius, spectra, carried, rates, ct, st, tth, ttl, vrad, vphi, radial_emb, azimuthal_emb
    )
    return (
        transported.reshape(rows, sector),
        kicked_r.reshape(rows, sector),
        kicked_p.reshape(rows, sector),
        push,
    )


def solution(mesh):
    placed = (P("rad", "az"), P("rad", "az"), P("rad", "az"), P("rad"), P(), P(), P())
    return jax.shard_map(
        on_device,
        mesh=mesh,
        in_specs=placed,
        out_specs=(P("rad", "az"), P("rad", "az"), P("rad", "az"), P()),
        check_vma=False,
    )
```
